32 devices in a mesh: data: 1 (over z), col: 4 (over y), row: 8 (over x, core).
Axes of the slice: x: 4, y: 4, z: 1, core: 2. Of those that a mesh axis runs over, the one named last changes fastest.
The devices are a block of a 4x4x8 slice.
Arguments:
- tokens: bfloat16 [4096, 6144], P(('data', 'row'), 'col')
- w_qkv: bfloat16 [6144, 8192], P('row', 'col')
- w_out: bfloat16 [6144, 6144], P('row', 'col')
- doc_ids: int32 [4096], P(('data', 'row'))
Outputs:
- output: bfloat16 [4096, 6144], P(('data', 'row'), 'col')
All inputs are finite; a program needn't handle non-finite values.
Results may differ from the reference program's by a relative error of at most 0.0039.
Values are sent between devices in bfloat16 or wider.
A program may use at most 768 MiB of HBM per device.

```python
import jax
import jax.numpy as jnp
from jax import lax

HIDDEN = 6144
N_HEADS = 48
KV_HEADS = 8
HEAD_DIM = 128
SEQ_LEN = 4096
N_DOCS = 4

GROUP_RATIO = N_HEADS // KV_HEADS
QKV_COLS = HIDDEN + 2 * KV_HEADS * HEAD_DIM


def block_size(row_count, score_width):
    q_blk = row_count
    while q_blk % 16 == 0 and q_blk * score_width > 4194304:
        q_blk = q_blk // 2
    return q_blk


def setup_inputs(seed: int = 0, part: int = 0) -> dict:
    base_key = jax.random.key(seed)
    key_qkv, key_out, key_part = jax.random.split(base_key, 3)
    part_key = jax.random.fold_in(key_part, part)
    key_tok, key_doc = jax.random.split(part_key)
    tokens = jax.random.normal(key_tok, (SEQ_LEN, HIDDEN), jnp.float32).astype(jnp.bfloat16)
    w_qkv = (jax.random.normal(key_qkv, (HIDDEN, QKV_COLS), jnp.float32) * HIDDEN ** -0.5).astype(jnp.bfloat16)
    w_out = (jax.random.normal(key_out, (HIDDEN, HIDDEN), jnp.float32) * HIDDEN ** -0.5).astype(jnp.bfloat16)
    doc_cuts = jax.random.randint(key_doc, (N_DOCS - 1,), 1, SEQ_LEN, dtype=jnp.int32)
    positions = jnp.arange(SEQ_LEN, dtype=jnp.int32)
    doc_ids = jnp.sum((positions[:, None] >= doc_cuts[None, :]).astype(jnp.int32), axis=1)
    return {"tokens": tokens, "w_qkv": w_qkv, "w_out": w_out, "doc_ids": doc_ids}


def reference(tokens, w_qkv, w_out, doc_ids):
    qkv_rows = jnp.dot(tokens, w_qkv, preferred_element_type=jnp.float32).astype(jnp.bfloat16)
    qkv_rows = qkv_rows.reshape(SEQ_LEN, KV_HEADS, GROUP_RATIO + 2, HEAD_DIM)
    key_rows = qkv_rows[:, :, GROUP_RATIO, :].astype(jnp.float32)
    value_rows = qkv_rows[:, :, GROUP_RATIO + 1, :].astype(jnp.float32)
    q_blk = block_size(SEQ_LEN, N_HEADS * SEQ_LEN)
    n_steps = SEQ_LEN // q_blk
    q_steps = qkv_rows[:, :, :GROUP_RATIO, :].reshape(n_steps, q_blk, KV_HEADS, GROUP_RATIO, HEAD_DIM)
    score_scale = HEAD_DIM ** -0.5

    def attend(block_in):
        q_part, seg_part = block_in
        scores = jnp.einsum("qgrd,kgd->qgrk", q_part.astype(jnp.float32), key_rows) * score_scale
        same_doc = seg_part[:, None, None, None] == doc_ids[None, None, None, :]
        scores = jnp.where(same_doc, scores, -jnp.inf)
        weights = jax.nn.softmax(scores, axis=-1).astype(jnp.bfloat16)
        context = jnp.einsum("qgrk,kgd->qgrd", weights.astype(jnp.float32), value_rows)
        return context.astype(jnp.bfloat16)

    context = lax.map(attend, (q_steps, doc_ids.reshape(n_steps, q_blk)))
    context = context.reshape(SEQ_LEN, HIDDEN)
    return jnp.dot(context, w_out, preferred_element_type=jnp.float32).astype(jnp.bfloat16)
```

```python
import functools
import math

import jax
import jax.numpy as jnp
from jax import lax
from jax.experimental import pallas as pl
from jax.experimental.pallas import tpu as pltpu
from jax.sharding import PartitionSpec as P

HEAD_DIM = 128
CHUNK = 256
MESH = pl.DeviceIdType.MESH
LOG2E = math.log2(math.e)
F32, BF16 = jnp.float32, jnp.bfloat16


def block_kernel(
    n_q, n_out,
    tokens, w_qkv, w_out, docs, out,
    wbuf, xbuf, obuf, kvbuf, qbuf, acc, score, stage, docbuf, doc_col,
    wl_sem, ws_sem, wr_sem, xl_sem, xs_sem, xr_sem, kvs_sem, kvr_sem,
    os_sem, or_sem, fl_sem, fs_sem, fr_sem, dl_sem, ds_sem, dr_sem,
):
    rows, k_dev = xbuf.shape[3], xbuf.shape[4]
    n_row = wbuf.shape[1]
    qkv_cols, out_cols = (n_q + 1) * CHUNK, n_out * CHUNK
    n_j = 1 + n_q + n_out

    me, y = lax.axis_index("row"), lax.axis_index("col")
    x, c = lax.div(me, 2), lax.rem(me, 2)
    other = 1 - c
    xr, xl, xo = lax.rem(x + 1, 4), lax.rem(x + 3, 4), lax.rem(x + 2, 4)
    yr, yl, yo = lax.rem(y + 1, 4), lax.rem(y + 3, 4), lax.rem(y + 2, 4)
    partner = {"row": 2 * x + other}
    x_right, x_left = {"row": 2 * xr + c}, {"row": 2 * xl + c}
    y_right, y_left = {"col": yr}, {"col": yl}

    def send(src, dst, s_sem, r_sem, device):
        return pltpu.make_async_remote_copy(
            src_ref=src, dst_ref=dst, send_sem=s_sem, recv_sem=r_sem,
            device_id=device, device_id_type=MESH)

    def same(ref, s_sem, r_sem, device):
        return send(ref, ref, s_sem, r_sem, device)

    def w_source(j, core):
        if j <= n_q:
            col = core * qkv_cols + (n_q * CHUNK if j == 0 else (j - 1) * CHUNK)
            return w_qkv.at[:, pl.ds(pl.multiple_of(col, 128), CHUNK)]
        col = core * out_cols + (j - 1 - n_q) * CHUNK
        return w_out.at[:, pl.ds(pl.multiple_of(col, 128), CHUNK)]

    def w_local(j):
        return pltpu.make_async_copy(w_source(j, c), wbuf.at[j, me], wl_sem.at[j])

    def w_pair(j):
        return send(w_source(j, other), wbuf.at[j, me], ws_sem.at[j, 4], wr_sem.at[j, 4], partner)

    def w_own(j):
        block = wbuf.at[j, pl.ds(2 * x, 2)]
        return (same(block, ws_sem.at[j, 0], wr_sem.at[j, 0], x_right),
                same(block, ws_sem.at[j, 1], wr_sem.at[j, 1], x_left))

    def w_fwd(j):
        return (same(wbuf.at[j, 2 * xl], ws_sem.at[j, 2], wr_sem.at[j, 2], x_right),
                same(wbuf.at[j, 2 * xr + 1], ws_sem.at[j, 3], wr_sem.at[j, 3], x_left))

    def x_local(h):
        return pltpu.make_async_copy(
            tokens.at[:, pl.ds(h * k_dev, k_dev)], xbuf.at[y, c, h], xl_sem.at[h])

    def x_right_own(h):
        return same(xbuf.at[y, c, h], xs_sem.at[h], xr_sem.at[h], y_right)

    def x_left_own(h):
        return same(xbuf.at[y, c, h], xs_sem.at[2 + h], xr_sem.at[2 + h], y_left)

    def x_fwd():
        return (same(xbuf.at[yl, c, 0], xs_sem.at[4], xr_sem.at[4], y_right),
                same(xbuf.at[yr, c, 1], xs_sem.at[5], xr_sem.at[5], y_left))

    def x_pair(k):
        ref = (xbuf.at[y, c], xbuf.at[yl, c], xbuf.at[yr, c], xbuf.at[yo, c, 0], xbuf.at[yo, c, 1])[k]
        return same(ref, xs_sem.at[6 + k], xr_sem.at[6 + k], partner)

    def kv_own():
        return (same(kvbuf.at[x], kvs_sem.at[0], kvr_sem.at[0], x_right),
                same(kvbuf.at[x], kvs_sem.at[1], kvr_sem.at[1], x_left))

    def kv_fwd():
        return (same(kvbuf.at[xl, 0], kvs_sem.at[2], kvr_sem.at[2], x_right),
                same(kvbuf.at[xr, 1], kvs_sem.at[3], kvr_sem.at[3], x_left))

    def o_own(p):
        ref = obuf.at[y, c, p]
        return (same(ref, os_sem.at[p, 0], or_sem.at[p, 0], y_right),
                same(ref, os_sem.at[p, 1], or_sem.at[p, 1], y_left))

    def o_fwd(p):
        return (same(obuf.at[yl, c, p, 0], os_sem.at[p, 2], or_sem.at[p, 2], y_right),
                same(obuf.at[yr, c, p, 1], os_sem.at[p, 3], or_sem.at[p, 3], y_left))

    def o_pair(p, k):
        ref = (obuf.at[y, c, p], obuf.at[yl, c, p], obuf.at[yr, c, p],
               obuf.at[yo, c, p, 0], obuf.at[yo, c, p, 1])[k]
        return same(ref, os_sem.at[p, 4 + k], or_sem.at[p, 4 + k], partner)

    def out_place(jj):
        return out.at[:, pl.ds(pl.multiple_of(c * out_cols + jj * CHUNK, 128), CHUNK)]

    def out_local(jj):
        return pltpu.make_async_copy(stage.at[jj, c], out_place(jj), fl_sem.at[jj])

    def out_pair(jj):
        return send(stage.at[jj, other], out_place(jj), fs_sem.at[jj], fr_sem.at[jj], partner)

    def doc_send(d):
        return same(docbuf.at[me], ds_sem.at[d - 1], dr_sem.at[d - 1], {"row": lax.rem(me + d, n_row)})

    def start(copies):
        for copy in copies:
            copy.start()

    def arrived(copies):
        for copy in copies:
            copy.wait_recv()

    def w_start_own(j):
        w_local(j).wait()
        w_pair(j).wait_recv()
        start(w_own(j))

    def w_relay(j):
        arrived(w_own(j))
        start(w_fwd(j))

    def chip_of(t):
        return lax.rem(x + t + lax.div(t, 2) * (5 - 2 * t), 4)

    def qkv_chunk(j, dst):
        acc[...] = jnp.zeros_like(acc)

        def step(t, carry):
            for half in range(2):
                total = jnp.dot(xbuf[t, half, 0], wbuf[j, 2 * t], preferred_element_type=F32)
                total += jnp.dot(xbuf[t, half, 1], wbuf[j, 2 * t + 1], preferred_element_type=F32)
                acc[half] += total
            return carry

        lax.fori_loop(0, 4, step, 0)
        dst[...] = acc[...].astype(BF16)

    def out_chunk(j, t0, t1):
        if t0 == 0:
            acc[...] = jnp.zeros_like(acc)

        def step(t, carry):
            chip = chip_of(t)
            for half in range(2):
                total = None
                for core in range(2):
                    for p in range(n_q):
                        part = jnp.dot(obuf[chip, core, p, half],
                                       wbuf[j, 2 * chip + core, p * CHUNK:(p + 1) * CHUNK, :],
                                       preferred_element_type=F32)
                        total = part if total is None else total + part
                acc[half] += total
            return carry

        lax.fori_loop(t0, t1, step, 0)

    def out_finish(jj):
        stage[jj] = acc[...].astype(BF16)
        out_pair(jj).start()
        out_local(jj).start()

    q_blk = score.shape[0]
    per_half = rows // q_blk
    tiles = rows // 128 if rows >= 128 else 1
    lanes = rows // tiles
    exp_scale = HEAD_DIM ** -0.5 * LOG2E

    def attend(p):
        def step(u, carry):
            half, r0 = lax.div(u, per_half), pl.multiple_of(lax.rem(u, per_half) * q_blk, q_blk)
            doc_q = doc_col[half, pl.ds(r0, q_blk), :]
            doc_q = jnp.concatenate([doc_q[:, :lanes]] * tiles, axis=1)
            for h in range(2):
                q = qbuf[half, pl.ds(r0, q_blk), h * HEAD_DIM:(h + 1) * HEAD_DIM]
                top = None
                for r in range(n_row):
                    k = kvbuf[r // 2, r % 2, :, :HEAD_DIM]
                    s = lax.dot_general(q, k, (((1,), (1,)), ((), ())), preferred_element_type=F32)
                    s = jnp.where(doc_q == docbuf[r], s, -jnp.inf)
                    score[:, r * rows:(r + 1) * rows] = s
                    for t in range(tiles):
                        part = s[:, t * lanes:(t + 1) * lanes]
                        top = part if top is None else jnp.maximum(top, part)
                top = jnp.max(top, axis=1, keepdims=True)
                total = None
                for r in range(n_row):
                    e = jnp.exp2((score[:, r * rows:(r + 1) * rows] - top) * exp_scale)
                    score[:, r * rows:(r + 1) * rows] = e
                    for t in range(tiles):
                        part = e[:, t * lanes:(t + 1) * lanes]
                        total = part if total is None else total + part
                inv = 1.0 / jnp.sum(total, axis=1, keepdims=True)
                o = None
                for r in range(n_row):
                    weights = (score[:, r * rows:(r + 1) * rows] * inv).astype(BF16)
                    part = jnp.dot(weights, kvbuf[r // 2, r % 2, :, HEAD_DIM:], preferred_element_type=F32)
                    o = part if o is None else o + part
                obuf[y, c, p, half, pl.ds(r0, q_blk), h * HEAD_DIM:(h + 1) * HEAD_DIM] = o.astype(BF16)
            return carry

        lax.fori_loop(0, 2 * per_half, step, 0)

    def o_start(p):
        start(o_own(p))
        o_pair(p, 0).start()

    def o_relay(p):
        right, left = o_own(p)
        f_right, f_left = o_fwd(p)
        right.wait_recv()
        f_right.start()
        o_pair(p, 1).start()
        left.wait_recv()
        f_left.start()
        o_pair(p, 2).start()

    def o_last(p):
        right, left = o_fwd(p)
        right.wait_recv()
        o_pair(p, 3).start()
        left.wait_recv()
        o_pair(p, 4).start()

    doc_load = pltpu.make_async_copy(docs, docbuf.at[me], dl_sem.at[0])
    for h in range(2):
        x_local(h).start()
    for j in range(n_j):
        w_local(j).start()
    doc_load.start()
    barrier = pltpu.get_barrier_semaphore()
    for d in range(1, n_row):
        pl.semaphore_signal(barrier, inc=1, device_id={"row": lax.rem(me + d, n_row)}, device_id_type=MESH)
    for device in (y_right, y_left):
        pl.semaphore_signal(barrier, inc=1, device_id=device, device_id_type=MESH)
    pl.semaphore_wait(barrier, n_row + 1)

    w_pair(0).start()
    x_local(0).wait()
    x_right_own(0).start()
    x_local(1).wait()
    x_left_own(1).start()
    x_right_own(1).start()
    x_left_own(0).start()
    w_pair(1).start()
    w_start_own(0)
    w_start_own(1)
    doc_load.wait()
    for d in range(1, n_row):
        doc_send(d).start()
    for j in range(2, n_j):
        w_pair(j).start()
    x_pair(0).start()

    x_fwd_right, x_fwd_left = x_fwd()
    x_right_own(0).wait_recv()
    x_fwd_right.start()
    x_left_own(1).wait_recv()
    x_fwd_left.start()
    w_relay(0)
    w_start_own(2)
    for d in range(1, n_row):
        doc_send(d).wait_recv()
    for core in range(2):
        row = docbuf[2 * x + core]
        doc_col[core] = jnp.transpose(jnp.broadcast_to(row, (128, rows)), (1, 0))
    x_right_own(1).wait_recv()
    x_pair(1).start()
    x_left_own(0).wait_recv()
    x_pair(2).start()
    w_relay(1)
    x_fwd_right.wait_recv()
    x_pair(3).start()
    x_fwd_left.wait_recv()
    x_pair(4).start()
    for k in range(5):
        x_pair(k).wait_recv()
    arrived(w_fwd(0))
    qkv_chunk(0, kvbuf.at[x])
    start(kv_own())
    w_relay(2)
    arrived(w_fwd(1))
    qkv_chunk(1, qbuf)
    arrived(kv_own())
    start(kv_fwd())
    w_start_own(3)
    w_start_own(4)
    arrived(kv_fwd())
    attend(0)
    o_start(0)
    w_relay(3)
    w_start_own(5)
    arrived(w_fwd(2))
    qkv_chunk(2, qbuf)
    attend(1)
    o_start(1)
    o_relay(0)
    w_relay(4)
    w_start_own(6)
    o_last(0)
    arrived(w_fwd(3))
    qkv_chunk(3, qbuf)
    attend(2)
    o_start(2)
    w_relay(5)
    o_relay(1)
    o_last(1)
    o_relay(2)
    o_last(2)
    w_relay(6)
    for p in range(n_q):
        for k in range(5):
            o_pair(p, k).wait_recv()
    arrived(w_fwd(4))
    out_chunk(4, 0, 4)
    out_finish(0)
    out_chunk(5, 0, 3)
    arrived(w_fwd(5))
    out_chunk(5, 3, 4)
    out_finish(1)
    out_chunk(6, 0, 3)
    arrived(w_fwd(6))
    out_chunk(6, 3, 4)
    out_finish(2)

    for j in range(n_j):
        w_pair(j).wait_send()
        for copy in w_own(j) + w_fwd(j):
            copy.wait_send()
    for h in range(2):
        x_right_own(h).wait_send()
        x_left_own(h).wait_send()
    for copy in x_fwd() + kv_own() + kv_fwd():
        copy.wait_send()
    for k in range(5):
        x_pair(k).wait_send()
    for p in range(n_q):
        for copy in o_own(p) + o_fwd(p):
            copy.wait_send()
        for k in range(5):
            o_pair(p, k).wait_send()
    for d in range(1, n_row):
        doc_send(d).wait_send()
    for jj in range(n_out):
        out_local(jj).wait()
        out_pair(jj).wait_send()
        out_pair(jj).wait_recv()


def solution(mesh):
    n_row, n_col = mesh.shape["row"], mesh.shape["col"]
    assert n_row == 2 * n_col

    def local_block(tokens, w_qkv, w_out, doc_ids):
        rows, _ = tokens.shape
        k_dev = w_qkv.shape[0]
        n_q = w_qkv.shape[1] // (2 * CHUNK) - 1
        n_out = w_out.shape[1] // (2 * CHUNK)
        n_j = 1 + n_q + n_out
        q_blk = min(256, rows)
        dma = pltpu.SemaphoreType.DMA
        any_spec = pl.BlockSpec(memory_space=pl.ANY)
        return pl.pallas_call(
            functools.partial(block_kernel, n_q, n_out),
            out_shape=jax.ShapeDtypeStruct(tokens.shape, BF16),
            in_specs=[any_spec] * 4,
            out_specs=any_spec,
            scratch_shapes=[
                pltpu.VMEM((n_j, n_row, k_dev, CHUNK), BF16),
                pltpu.VMEM((n_col, 2, 2, rows, k_dev), BF16),
                pltpu.VMEM((n_col, 2, n_q, 2, rows, CHUNK), BF16),
                pltpu.VMEM((n_col, 2, rows, CHUNK), BF16),
                pltpu.VMEM((2, rows, CHUNK), BF16),
                pltpu.VMEM((2, rows, CHUNK), F32),
                pltpu.VMEM((q_blk, n_row * rows), F32),
                pltpu.VMEM((n_out, 2, rows, CHUNK), BF16),
                pltpu.VMEM((n_row, 1, rows), jnp.int32),
                pltpu.VMEM((2, rows, 128), jnp.int32),
                dma((n_j,)), dma((n_j, 5)), dma((n_j, 5)),
                dma((2,)), dma((11,)), dma((11,)),
                dma((4,)), dma((4,)),
                dma((n_q, 9)), dma((n_q, 9)),
                dma((n_out,)), dma((n_out,)), dma((n_out,)),
                dma((1,)), dma((n_row - 1,)), dma((n_row - 1,)),
            ],
            compiler_params=pltpu.CompilerParams(
                collective_id=0, has_side_effects=True, vmem_limit_bytes=67043328),
            name="attention_block",
        )(tokens, w_qkv, w_out, doc_ids.reshape(1, rows))

    row_spec = P(("data", "row"), "col")
    weight_spec = P("row", "col")
    return jax.shard_map(local_block, mesh=mesh, in_specs=(row_spec, weight_spec, weight_spec, P(("data", "row"))),
                         out_specs=row_spec, check_vma=False)
```

```python
import functools
import math
from types import SimpleNamespace

import jax
import jax.numpy as jnp
from jax import lax
from jax.experimental import pallas as pl
from jax.experimental.pallas import tpu as pltpu
from jax.sharding import PartitionSpec as P

HEAD_DIM = 128
CHUNK = 256
MESH = pl.DeviceIdType.MESH
LOG2E = math.log2(math.e)
F32, BF16 = jnp.float32, jnp.bfloat16


def block_kernel(
    n_q, n_out,
    tokens, w_qkv, w_out, docs, out,
    wq, wo, xbuf, obuf, kvbuf, qbuf, acc, score, docbuf, doc_col,
    ql_sem, qs_sem, qr_sem, wl_sem, ws_sem, wr_sem, xl_sem, xs_sem, xr_sem,
    ks_sem, kr_sem, os_sem, or_sem, fl_sem, fs_sem, fr_sem, dl_sem, ds_sem, dr_sem,
):
    rows, k_dev = xbuf.shape[3], xbuf.shape[4]
    n_row = wq.shape[1]
    qkv_cols, out_cols = (n_q + 1) * CHUNK, n_out * CHUNK
    n_j = 1 + n_q
    split = rows // 2

    me, y = lax.axis_index("row"), lax.axis_index("col")
    x, c = lax.div(me, 2), lax.rem(me, 2)
    group = lax.div(x, 2)
    near, mate = x + 1 - 2 * lax.rem(x, 2), 3 - x
    far = 3 - near
    yr, yl, yo = (lax.rem(y + d, 4) for d in (1, 3, 2))
    partner = {"row": 2 * x + 1 - c}
    to_near, to_mate = {"row": 2 * near + c}, {"row": 2 * mate + c}
    right, left = {"col": yr}, {"col": yl}
    others = [lax.rem(me + d, n_row) for d in range(1, n_row)]

    started = []

    def go(*copies):
        for copy in copies:
            copy.start()
            started.append(copy)

    def arrived(*copies):
        for copy in copies:
            copy.wait_recv()

    def make(source, place, s_sem, r_sem, device):
        return pltpu.make_async_remote_copy(
            src_ref=source, dst_ref=place, send_sem=s_sem, recv_sem=r_sem,
            device_id=device, device_id_type=MESH)

    def remote(s_sem, r_sem, **table):
        made = {}
        for i, (name, entry) in enumerate(table.items()):
            made[name] = make(entry[0], entry[-2], s_sem.at[i], r_sem.at[i], entry[-1])
        return SimpleNamespace(**made)

    def q_source(j, g):
        col = g * qkv_cols + (n_q if j == 0 else j - 1) * CHUNK
        return w_qkv.at[:, pl.ds(pl.multiple_of(col, 128), CHUNK)]

    def q_copies(j):
        near_block, mate_block, far_block = (wq.at[j, 2 * chip + c] for chip in (near, mate, far))
        return remote(
            qs_sem.at[j], qr_sem.at[j],
            near=(q_source(j, group), wq.at[j, me], to_near),
            mate=(q_source(j, 1 - group), wq.at[j, me], to_mate),
            relay=(mate_block, to_near),
            pair_own=(q_source(j, group), wq.at[j, me], partner),
            pair_near=(near_block, partner),
            pair_mate=(mate_block, partner),
            pair_far=(far_block, partner))

    def w_source(j, core):
        col = core * out_cols + j * CHUNK
        return w_out.at[:, pl.ds(pl.multiple_of(col, 128), CHUNK)]

    def w_copies(j):
        block_a, block_b = wo.at[j, 2 * x], wo.at[j, 2 * x + 1]
        copies = dict(
            near_a=(block_a, to_near), near_b=(block_b, to_near),
            mate_a=(block_a, to_mate), mate_b=(block_b, to_mate),
            pair=(w_source(j, 1 - c), wo.at[j, me], partner),
            relay_a=(wo.at[j, 2 * mate], to_near))
        if j == n_out - 1:
            copies.update(relay_b=(wo.at[j, 2 * mate + 1], to_near))
        else:
            copies.update(relay_b=(wo.at[j, 2 * near + 1], to_mate))
        return remote(ws_sem.at[j], wr_sem.at[j], **copies)

    def x_half(h):
        return tokens.at[:, pl.ds(h * k_dev, k_dev)]

    x_own = remote(
        xs_sem.at[0], xr_sem.at[0],
        right0=(xbuf.at[0, y, 0], right), left1=(xbuf.at[0, y, 1], left),
        right1=(xbuf.at[0, y, 1], right), left0=(xbuf.at[0, y, 0], left),
        relay_right=(xbuf.at[0, yl, 0], right), relay_left=(xbuf.at[0, yr, 1], left),
        mate0=(x_half(0), xbuf.at[1, y, 0], to_mate), mate1=(x_half(1), xbuf.at[1, y, 1], to_mate))
    x_far = (xbuf.at[s, yo, :, pl.ds(split, split)] for s in range(2))
    x_mate = remote(
        xs_sem.at[1], xr_sem.at[1],
        right0=(xbuf.at[1, y, 0], right), left1=(xbuf.at[1, y, 1], left),
        right1=(xbuf.at[1, y, 1], right), left0=(xbuf.at[1, y, 0], left),
        relay_right=(xbuf.at[1, yl, 0, pl.ds(0, split)], right),
        relay_left=(xbuf.at[1, yr, 1, pl.ds(0, split)], left),
        far=(*x_far, to_mate))

    kv = remote(
        ks_sem, kr_sem,
        own=(kvbuf.at[x, c], to_near), mate=(kvbuf.at[mate, c], to_near),
        pair_own=(kvbuf.at[x, c], partner), pair_mate=(kvbuf.at[mate, c], partner),
        pair_near=(kvbuf.at[near, c], partner), pair_far=(kvbuf.at[far, c], partner))

    def o_copies(p):
        def place(col):
            return obuf.at[col, p, c, 1 - group], obuf.at[col, p, c, group]

        first, second = place(y)
        first_l, second_l = place(yl)
        first_r, second_r = place(yr)
        first_o, second_o = place(yo)
        return remote(
            os_sem.at[p], or_sem.at[p],
            back=(qbuf.at[p, 1], second, to_mate),
            first_right=(first, right), first_left=(first, left),
            second_right=(second, right), second_left=(second, left),
            relay_right=(first_l, right), relay_left=(second_r, left),
            pair_first=(first, partner), pair_second=(second, partner),
            pair_first_l=(first_l, partner), pair_second_l=(second_l, partner),
            pair_first_r=(first_r, partner), pair_second_r=(second_r, partner),
            pair_first_o=(first_o, partner), pair_second_o=(second_o, partner))

    def out_place(j):
        return out.at[:, pl.ds(pl.multiple_of(c * out_cols + j * CHUNK, 128), CHUNK)]

    out_local = [pltpu.make_async_copy(qbuf.at[j, c], out_place(j), fl_sem.at[j]) for j in range(n_out)]
    out_pair = [make(qbuf.at[j, 1 - c], out_place(j), fs_sem.at[j], fr_sem.at[j], partner) for j in range(n_out)]
    doc = [make(docbuf.at[me], docbuf.at[me], ds_sem.at[i], dr_sem.at[i], {"row": other})
           for i, other in enumerate(others)]

    q = [q_copies(j) for j in range(n_j)]
    w = [w_copies(j) for j in range(n_out)]
    o = [o_copies(p) for p in range(n_q)]

    def order(i, t):
        return lax.rem(i + t + lax.div(t, 2) * (5 - 2 * t), 4)

    def clear(i):
        acc[i] = jnp.zeros(acc.shape[1:], F32)

    def qkv_part(s, j, t0, t1):
        if t0 == 0:
            clear(j)

        def step(t, carry):
            col = order(y, t)
            total = jnp.dot(xbuf[s, col, 0], wq[j, 2 * col], preferred_element_type=F32)
            total += jnp.dot(xbuf[s, col, 1], wq[j, 2 * col + 1], preferred_element_type=F32)
            acc[j] += total
            return carry

        lax.fori_loop(t0, t1, step, 0)

    def qkv_store(s, j):
        value = acc[j].astype(BF16)
        if j == 0:
            kvbuf[mate if s else x, c] = value
        else:
            qbuf[j - 1, s] = value

    def out_part(j, start_at, t0, t1, p0, p1):
        if t0 == 0 and p0 == 0:
            clear(2 * j)
            clear(2 * j + 1)

        def step(t, carry):
            col = order(start_at, t)
            for half in range(2):
                total = None
                for g in range(2):
                    for p in range(p0, p1):
                        part = jnp.dot(obuf[col, p, half, g],
                                       wo[j, 2 * col + g, p * CHUNK:(p + 1) * CHUNK, :],
                                       preferred_element_type=F32)
                        total = part if total is None else total + part
                acc[2 * j + half] += total
            return carry

        lax.fori_loop(t0, t1, step, 0)

    def out_finish(j):
        qbuf[j] = acc[2 * j:2 * j + 2].astype(BF16)
        go(out_pair[j])
        out_local[j].start()

    q_blk = score.shape[1]
    per_s = rows // q_blk
    tiles = rows // 128 if rows >= 128 else 1
    lanes = rows // tiles
    exp_scale = HEAD_DIM ** -0.5 * LOG2E

    def query(s, p, u):
        h, r0 = lax.div(u, per_s), pl.multiple_of(lax.rem(u, per_s) * q_blk, q_blk)
        head = pl.ds(pl.multiple_of(h * HEAD_DIM, HEAD_DIM), HEAD_DIM)
        doc_q = doc_col[s, pl.ds(r0, q_blk), :]
        return qbuf[p, s, pl.ds(r0, q_blk), head], jnp.concatenate([doc_q[:, :lanes]] * tiles, axis=1)

    def fold(op, value, total):
        for t in range(tiles):
            part = value[:, t * lanes:(t + 1) * lanes]
            total = part if total is None else op(total, part)
        return total

    def scores(slot, r, q, doc_q, top):
        k = kvbuf[r // 2, r % 2, :, :HEAD_DIM]
        sc = lax.dot_general(q, k, (((1,), (1,)), ((), ())), preferred_element_type=F32)
        sc = jnp.where(doc_q == docbuf[r], sc, -jnp.inf)
        score[slot, :, r * rows:(r + 1) * rows] = sc
        return fold(jnp.maximum, sc, top)

    def first_scores(s, p):
        q, doc_q = query(s, p, 0)
        top = None
        for r in range(n_row):
            top = scores(0, r, q, doc_q, top)
        return jnp.max(top, axis=1, keepdims=True)

    def unit(slot, top, s, p, u, s_b, p_b, u_b):
        q, doc_q = query(s_b, p_b, u_b)
        top_b, total = None, None
        for r in range(n_row):
            part = slice(r * rows, (r + 1) * rows)
            e = jnp.exp2((score[slot, :, part] - top) * exp_scale)
            score[slot, :, part] = e
            total = fold(jnp.add, e, total)
            top_b = scores(1 - slot, r, q, doc_q, top_b)
        inv = 1.0 / jnp.sum(total, axis=1, keepdims=True)
        o = None
        for r in range(n_row):
            weights = (score[slot, :, r * rows:(r + 1) * rows] * inv).astype(BF16)
            part = jnp.dot(weights, kvbuf[r // 2, r % 2, :, HEAD_DIM:], preferred_element_type=F32)
            o = part if o is None else o + part
        o = o.astype(BF16)
        h, r0 = lax.div(u, per_s), pl.multiple_of(lax.rem(u, per_s) * q_blk, q_blk)
        head = pl.ds(pl.multiple_of(h * HEAD_DIM, HEAD_DIM), HEAD_DIM)

        @pl.when(s == 1)
        def _():
            qbuf[p, 1, pl.ds(r0, q_blk), head] = o

        @pl.when(s == 0)
        def _():
            obuf[y, p, c, group, pl.ds(r0, q_blk), head] = o

        return jnp.max(top_b, axis=1, keepdims=True)

    doc_load = pltpu.make_async_copy(docs, docbuf.at[me], dl_sem.at[0])
    x_load = [pltpu.make_async_copy(x_half(h), xbuf.at[0, y, h], xl_sem.at[h]) for h in range(2)]
    q_load = [pltpu.make_async_copy(q_source(j, group), wq.at[j, me], ql_sem.at[j]) for j in range(n_j)]
    w_load = [pltpu.make_async_copy(w_source(j, c), wo.at[j, me], wl_sem.at[j]) for j in range(n_out)]
    for load in [doc_load] + x_load + q_load + w_load:
        load.start()
    barrier = pltpu.get_barrier_semaphore()
    for device in [{"row": other} for other in others] + [right, left]:
        pl.semaphore_signal(barrier, inc=1, device_id=device, device_id_type=MESH)
    pl.semaphore_wait(barrier, n_row + 1)

    doc_load.wait()
    go(*doc)
    go(x_own.mate0, x_own.mate1, q[0].near)
    x_load[0].wait()
    go(x_own.right0)
    x_load[1].wait()
    go(x_own.left1, x_own.right1, x_own.left0)
    go(*(copies.mate for copies in q))
    go(*(copies.near for copies in q[1:]))
    go(*(copies.pair_own for copies in q))
    go(*(copies.pair for copies in w))

    def w_ready(j):
        w_load[j].wait()
        arrived(w[j].pair)

    w_ready(0)
    go(w[0].near_a, w[0].near_b)
    for load in q_load:
        load.wait()
    arrived(*doc)
    for s in range(2):
        row = docbuf[2 * (mate if s else x) + c]
        doc_col[s] = jnp.transpose(jnp.broadcast_to(row, (128, rows)), (1, 0))

    def pass_on(*pairs):
        for there, onward in pairs:
            arrived(there)
            go(onward)

    pass_on((x_own.right0, x_own.relay_right), (x_own.left1, x_own.relay_left),
            (x_own.mate0, x_mate.right0))
    pass_on(*((copies.near, copies.pair_near) for copies in q[:2]))
    arrived(x_own.mate1)
    go(x_mate.left1, x_mate.right1, x_mate.left0)
    pass_on(*((copies.near, copies.pair_near) for copies in q[2:]))
    arrived(x_own.right1, x_own.left0)

    def q_relay(j):
        pass_on((q[j].mate, q[j].relay))
        go(q[j].pair_mate)

    def q_done(j):
        pass_on((q[j].relay, q[j].pair_far))
        arrived(q[j].pair_own, q[j].pair_near, q[j].pair_mate, q[j].pair_far)

    q_relay(0)
    arrived(x_own.relay_right, x_own.relay_left)
    go(x_mate.far)
    q_relay(1)
    q_done(0)
    qkv_part(0, 0, 0, 4)
    qkv_store(0, 0)
    q_relay(2)
    go(w[0].mate_a, w[0].mate_b)
    q_relay(3)
    go(kv.own, kv.pair_own)
    pass_on((x_mate.right0, x_mate.relay_right), (x_mate.left1, x_mate.relay_left))
    w_ready(1)
    go(w[1].mate_a)
    for j in range(1, n_j):
        q_done(j)
        qkv_part(0, j, 0, 4)
        qkv_store(0, j)
    arrived(x_mate.right1, x_mate.left0)
    pass_on((kv.own, kv.pair_near))
    for j in range(n_j):
        qkv_part(1, j, 0, 3)
    w_ready(2)
    arrived(x_mate.far, x_mate.relay_right, x_mate.relay_left)
    for j in range(n_j):
        qkv_part(1, j, 3, 4)
        if j == 1:
            go(kv.mate, kv.pair_mate)
        qkv_store(1, j)
    go(w[1].near_a, w[1].near_b, w[2].near_a, w[2].near_b)
    pass_on((w[0].mate_a, w[0].relay_a), (kv.mate, kv.pair_far))
    arrived(kv.pair_own, kv.pair_mate, kv.pair_near, kv.pair_far)

    def o_first(p):
        arrived(o[p].back)
        go(o[p].first_right, o[p].first_left, o[p].pair_first)

    def o_second(p):
        go(o[p].second_right, o[p].second_left, o[p].pair_second)

    def o_relay(p, is_first):
        if is_first:
            pass_on((o[p].first_right, o[p].relay_right))
        else:
            pass_on((o[p].second_left, o[p].relay_left))

    def o_share(p, is_first):
        if is_first:
            go(o[p].pair_first_l)
            pass_on((o[p].first_left, o[p].pair_first_r))
        else:
            go(o[p].pair_second_r)
            pass_on((o[p].second_right, o[p].pair_second_l))

    def o_last(p):
        pass_on((o[p].relay_right, o[p].pair_first_o), (o[p].relay_left, o[p].pair_second_o))

    def o_done(p, last):
        if last:
            arrived(o[p].pair_first_o, o[p].pair_second_o)
        else:
            arrived(o[p].pair_first, o[p].pair_second, o[p].pair_first_l, o[p].pair_second_l,
                    o[p].pair_first_r, o[p].pair_second_r)

    def after_0():
        go(o[0].back, w[1].mate_b)
        pass_on((w[1].mate_a, w[1].relay_a))

    def after_1():
        o_second(0)
        o_first(0)

    def after_2():
        go(o[1].back, w[2].mate_a)
        o_relay(0, False)

    def after_3():
        o_relay(0, True)
        o_second(1)
        o_first(1)
        o_share(0, False)
        o_share(0, True)
        arrived(w[0].near_b)
        go(w[0].relay_b)

    def after_4():
        arrived(w[1].near_b)
        go(o[2].back, w[2].mate_b, w[1].relay_b)

    def attend(i, top):
        step, u = lax.div(i, 2), per_s * lax.rem(i, 2)
        s, p = 1 - lax.rem(step, 2), lax.div(step, 2)
        later = jnp.minimum(i + 1, 4 * n_q - 1)
        step_b, u_b = lax.div(later, 2), per_s * lax.rem(later, 2)
        top = unit(0, top, s, p, u, s, p, u + 1)
        top = unit(1, top, s, p, u + 1, 1 - lax.rem(step_b, 2), lax.div(step_b, 2), u_b)
        for k, hook in enumerate((after_0, after_1, after_2, after_3, after_4)):
            pl.when(i == 2 * k + 1)(hook)
        pl.when(i == 4 * n_q - 2)(lambda: o_relay(1, False))
        return top

    lax.fori_loop(0, 4 * n_q, attend, first_scores(1, 0))
    o_second(2)
    pass_on((w[2].mate_a, w[2].relay_a))
    o_last(0)
    o_share(1, False)
    o_relay(1, True)
    o_share(1, True)
    o_done(0, False)
    o_done(0, True)
    arrived(w[0].mate_b, w[0].near_a, w[0].relay_a, w[0].relay_b)
    out_part(0, y, 0, 4, 0, 1)
    o_first(2)
    o_relay(2, False)
    arrived(w[1].mate_b, w[1].near_a, w[2].near_a, w[2].near_b)
    o_last(1)
    pass_on((w[2].mate_b, w[2].relay_b))
    o_done(1, False)
    o_done(1, True)
    out_part(0, y, 0, 4, 1, 2)
    out_part(1, x, 0, 3, 0, 2)
    o_relay(2, True)
    o_share(2, False)
    o_share(2, True)
    out_part(2, x, 0, 3, 0, 2)
    o_done(2, False)
    out_part(0, y, 0, 3, 2, 3)
    arrived(w[1].relay_a, w[1].relay_b)
    out_part(1, x, 3, 4, 0, 2)
    out_part(1, y, 0, 3, 2, 3)
    o_last(2)
    arrived(w[2].relay_a, w[2].relay_b)
    out_part(2, x, 3, 4, 0, 2)
    out_part(2, y, 0, 3, 2, 3)
    o_done(2, True)
    for copies in o:
        copies.back.wait_send()
    for j in range(n_out):
        out_part(j, y, 3, 4, 2, 3)
        out_finish(j)

    for copy in started:
        if not any(copy is copies.back for copies in o):
            copy.wait_send()
    for copy in out_local:
        copy.wait()
    arrived(*out_pair)


def solution(mesh):
    n_row, n_col = mesh.shape["row"], mesh.shape["col"]
    assert n_row == 2 * n_col

    def local_block(tokens, w_qkv, w_out, doc_ids):
        rows, _ = tokens.shape
        k_dev = w_qkv.shape[0]
        n_q = w_qkv.shape[1] // (2 * CHUNK) - 1
        n_out = w_out.shape[1] // (2 * CHUNK)
        n_j = 1 + n_q
        q_blk = min(256, rows)
        dma = pltpu.SemaphoreType.DMA
        any_spec = pl.BlockSpec(memory_space=pl.ANY)
        return pl.pallas_call(
            functools.partial(block_kernel, n_q, n_out),
            out_shape=jax.ShapeDtypeStruct(tokens.shape, BF16),
            in_specs=[any_spec] * 4,
            out_specs=any_spec,
            scratch_shapes=[
                pltpu.VMEM((n_j, n_row, k_dev, CHUNK), BF16),
                pltpu.VMEM((n_out, n_row, k_dev, CHUNK), BF16),
                pltpu.VMEM((2, n_col, 2, rows, k_dev), BF16),
                pltpu.VMEM((n_col, n_q, 2, 2, rows, CHUNK), BF16),
                pltpu.VMEM((n_col, 2, rows, CHUNK), BF16),
                pltpu.VMEM((n_q, 2, rows, CHUNK), BF16),
                pltpu.VMEM((max(n_j, 2 * n_out), rows, CHUNK), F32),
                pltpu.VMEM((2, q_blk, n_row * rows), F32),
                pltpu.VMEM((n_row, 1, rows), jnp.int32),
                pltpu.VMEM((2, rows, 128), jnp.int32),
                dma((n_j,)), dma((n_j, 7)), dma((n_j, 7)),
                dma((n_out,)), dma((n_out, 7)), dma((n_out, 7)),
                dma((2,)), dma((2, 8)), dma((2, 8)),
                dma((6,)), dma((6,)),
                dma((n_q, 15)), dma((n_q, 15)),
                dma((n_out,)), dma((n_out,)), dma((n_out,)),
                dma((1,)), dma((n_row - 1,)), dma((n_row - 1,)),
            ],
            compiler_params=pltpu.CompilerParams(
                collective_id=0, has_side_effects=True, vmem_limit_bytes=67043328),
            name="attention_block",
        )(tokens, w_qkv, w_out, doc_ids.reshape(1, rows))

    row_spec = P(("data", "row"), "col")
    weight_spec = P("row", "col")
    return jax.shard_map(local_block, mesh=mesh, in_specs=(row_spec, weight_spec, weight_spec, P(("data", "row"))),
                         out_specs=row_spec, check_vma=False)
```
